32 devices in a mesh: dp: 8 (over z, x), expert: 4 (over y, core).
Axes of the slice: x: 2, y: 2, z: 4, core: 2. Of those that a mesh axis runs over, the one named last changes fastest.
Arguments:
- tokens: bfloat16 [512, 2048], P('expert'), may hold values from -6 to 6
- cotangent: bfloat16 [512, 2048], P('expert'), may hold values from -0.75 to 0.75
- router_logits: float32 [512, 2], P('expert'), may hold values from -6 to 6
- routes: int32 [512, 2], P('expert'), may hold values from 0 to 3, all different within a row; in each aligned block of 128 rows (0 to 127, 128 to 255, ...) at most 96 rows name the same one
- gate_weight: bfloat16 [4, 7168, 2048], P('expert', 'dp'), may hold values from -0.125 to 0.125
- up_weight: bfloat16 [4, 7168, 2048], P('expert', 'dp'), may hold values from -0.125 to 0.125
- down_weight: bfloat16 [4, 7168, 2048], P('expert', 'dp'), may hold values from -0.0625 to 0.0625
- dir_gate: bfloat16 [4, 7168, 2048], P('expert', 'dp'), may hold values from -0.125 to 0.125
- dir_up: bfloat16 [4, 7168, 2048], P('expert', 'dp'), may hold values from -0.125 to 0.125
- dir_down: bfloat16 [4, 7168, 2048], P('expert', 'dp'), may hold values from -0.0625 to 0.0625
Outputs:
- mixed: bfloat16 [512, 2048], P('expert')
- hvp_gate: float32 [4, 7168, 2048], P('expert', 'dp')
- hvp_up: float32 [4, 7168, 2048], P('expert', 'dp')
- hvp_down: float32 [4, 7168, 2048], P('expert', 'dp')
The draws below stay inside these ranges and needn't reach their ends.
Inputs may be any that keep to these rules, and one draw needn't show every extreme that they name: `routes`: each row names 2 different experts; among the 128 rows of one index of the expert axis no expert is named more than 96 times, and in every draw some block names some expert exactly 96 times.
All inputs are finite; a program needn't handle non-finite values.
Results may differ from the reference program's by a relative error of at most 0.0074.
Values may be sent and summed in bfloat16 or wider, within the bound.
A program may use at most 128 MiB of HBM per device.

```python
import math
import jax
import jax.numpy as jnp
import numpy as np
from jax import lax

D = 2048
FF = 7168
TOP = 2
TOK_DEV = 128
EXPERTS = 4
CAP = 96
TOKENS = 512


def levels(own_key, extent, shards, least, largest):
    loudness, own = 1.0, jax.random.fold_in(own_key, 6)
    for position, blocks in shards:
        heights = jnp.exp(jax.random.uniform(jax.random.fold_in(own, position), (blocks,), jnp.float32, least / len(shards), largest / len(shards)))
        loudness = loudness * jnp.repeat(heights, extent[position] // blocks).reshape([-1 if axis == position else 1 for axis in range(len(extent))])
    return loudness


def assign_block(key, own, number, rows, amount, top, most, lean):
    order = jax.random.permutation(key, amount)
    crowded, usual = shares(amount, rows * top, most, lean, True), shares(amount, rows * top, most, lean, False)
    places = jnp.arange(amount)

    def named(lengths, rotation):
        used = int((lengths > 0).sum())
        fixed = max(1, used // 4)
        moved = fixed + (places - fixed + rotation * (used - fixed)) % max(1, amount - fixed)
        return jnp.zeros((amount,), jnp.int32).at[order[jnp.where(places < fixed, places, moved)]].set(jnp.asarray(lengths, jnp.int32))

    lengths = jnp.where(number % 4 == 0, named(crowded, number // 4), named(usual, number - number // 4 - 1))
    mixed = jax.random.permutation(jax.random.fold_in(own, 3), amount)
    source_of, sink = mixed[0:amount // 2 * 2:2], mixed[1:amount // 2 * 2:2]
    room = jnp.minimum(lengths[source_of] - 1, most - lengths[sink]) // 2
    room = jnp.where((source_of == order[0]) | (sink == order[0]) | (lengths[sink] == 0), 0, jnp.maximum(room, 0))
    moved = jax.random.randint(jax.random.fold_in(own, 4), (amount // 2,), 0, 1 << 20) % (room + 1)
    lengths = lengths.at[source_of].add(-moved).at[sink].add(moved)
    labels = jnp.searchsorted(jnp.cumsum(lengths), jnp.arange(rows * top), side="right").astype(jnp.int32)
    grid = labels.reshape(top, rows).T
    grid = grid[jax.random.permutation(jax.random.fold_in(own, 1), rows)]
    rotation = jax.random.randint(jax.random.fold_in(own, 2), (rows, 1), 0, top)
    return jnp.take_along_axis(grid, (jnp.arange(top)[None, :] + rotation) % top, axis=1)


def shares(count, total, reach, skew, full):
    portions = [(1 << 20) // math.isqrt(grade ** skew) + 1 for grade in range(1, count + 1)]
    largest = reach if full else min(reach, max(-(-total // count), total * portions[0] // sum(portions)))
    least = 1 if total - largest >= count - 1 else 0
    holding, spare = [largest] + [least] * (count - 1), total - largest - least * (count - 1)
    while spare > 0:
        candidates = [i for i in range(1, count) if holding[i] < largest] or [i for i in range(1, count) if holding[i] < reach]
        whole, left = sum([portions[i] for i in candidates]), spare
        for i in candidates:
            extra = min(reach - holding[i], max(1, left * portions[i] // whole), spare)
            holding[i] = holding[i] + extra
            spare = spare - extra
    return np.array(holding)


def gaussian(key, shape, width, most, shards=(), kind=jnp.bfloat16):
    array = width * jax.random.normal(key, shape, jnp.float32)
    if shards:
        array = array * levels(key, shape, shards, -0.22, 0.18)
    return jnp.clip(array, -most, most).astype(kind)


def setup_inputs(seed: int = 0) -> dict:
    seeds = jax.random.split(jax.random.key(seed), 11)
    tokens = gaussian(seeds[0], (TOKENS, D), 1.0, 6.0, ((0, 4),))
    cotangent = gaussian(seeds[1], (TOKENS, D), 0.125, 0.75, ((0, 4),))
    router_logits = gaussian(seeds[2], (TOKENS, TOP), 1.0, 6.0, ((0, 4),), jnp.float32)
    routes_keys = jax.random.split(jax.random.fold_in(seeds[3], 1), TOKENS // TOK_DEV)
    routes_turns = jax.random.permutation(jax.random.fold_in(seeds[3], 3), TOKENS // TOK_DEV)
    routes = jax.vmap(lambda own, number: assign_block(jax.random.fold_in(seeds[3], 2), own, number, TOK_DEV, EXPERTS, TOP, CAP, 2))(routes_keys, routes_turns).reshape((TOKENS, TOP))
    gate_weight = gaussian(seeds[4], (EXPERTS, FF, D), D ** -0.5, 0.125, ((0, 4), (1, 8)))
    up_weight = gaussian(seeds[5], (EXPERTS, FF, D), D ** -0.5, 0.125, ((0, 4), (1, 8)))
    down_weight = gaussian(seeds[6], (EXPERTS, FF, D), FF ** -0.5, 0.0625, ((0, 4), (1, 8)))
    dir_gate = gaussian(seeds[7], (EXPERTS, FF, D), D ** -0.5, 0.125, ((0, 4), (1, 8)))
    dir_up = gaussian(seeds[8], (EXPERTS, FF, D), D ** -0.5, 0.125, ((0, 4), (1, 8)))
    dir_down = gaussian(seeds[9], (EXPERTS, FF, D), FF ** -0.5, 0.0625, ((0, 4), (1, 8)))
    return dict(tokens=tokens, cotangent=cotangent, router_logits=router_logits, routes=routes, gate_weight=gate_weight, up_weight=up_weight, down_weight=down_weight, dir_gate=dir_gate, dir_up=dir_up, dir_down=dir_down)


def derivatives(preact):
    sigmoid_value = jax.nn.sigmoid(preact)
    slope_one = sigmoid_value * (1.0 + preact * (1.0 - sigmoid_value))
    slope_two = sigmoid_value * (1.0 - sigmoid_value) * (2.0 + preact * (1.0 - 2.0 * sigmoid_value))
    return preact * sigmoid_value, slope_one, slope_two


def project(left_rows, matrix):
    return jnp.einsum("rd,hd->rh", left_rows, matrix, preferred_element_type=jnp.float32)


def outer_sum(left_rows, right_rows):
    return jnp.einsum("rh,rd->hd", left_rows, right_rows, preferred_element_type=jnp.float32)


def block_terms(weights, token_rows, cot_rows):
    gate_mat, up_mat, down_mat, gate_dir, up_dir, down_dir = weights
    preact = project(token_rows, gate_mat)
    up_value = project(token_rows, up_mat)
    back_grad = project(cot_rows, down_mat)
    tang_gate = project(token_rows, gate_dir)
    tang_up = project(token_rows, up_dir)
    back_tang = project(cot_rows, down_dir)
    silu_value, slope_one, slope_two = derivatives(preact)
    hidden = (silu_value * up_value).astype(jnp.bfloat16)
    silu_tang = slope_one * tang_gate
    hidden_tang = (silu_tang * up_value + silu_value * tang_up).astype(jnp.bfloat16)
    resid_gate = ((back_tang * up_value + back_grad * tang_up) * slope_one + back_grad * up_value * slope_two * tang_gate).astype(jnp.bfloat16)
    resid_up = (back_tang * silu_value + back_grad * silu_tang).astype(jnp.bfloat16)
    return hidden, outer_sum(resid_gate, token_rows), outer_sum(resid_up, token_rows), outer_sum(hidden_tang, cot_rows)


def reference(tokens, cotangent, router_logits, routes, gate_weight, up_weight, down_weight, dir_gate, dir_up, dir_down):
    sources = TOKENS // TOK_DEV
    gate_first = jax.nn.sigmoid(router_logits[:, 0] - router_logits[:, 1])
    gate_prob = jnp.stack([gate_first, 1.0 - gate_first], axis=1)
    onehot = (routes.reshape(sources, TOK_DEV * TOP)[:, :, None] == jnp.arange(EXPERTS, dtype=jnp.int32)[None, None, :]).astype(jnp.int32)
    earlier = jnp.cumsum(onehot, axis=1) - onehot
    slot_pos = jnp.sum(earlier * onehot, axis=2).reshape(TOKENS, TOP)
    source = (jnp.arange(TOKENS, dtype=jnp.int32) // TOK_DEV)[:, None]
    slot_index = ((routes * sources + source) * CAP + slot_pos).reshape(-1).astype(jnp.int32)
    scaled = (gate_prob[:, :, None] * cotangent.astype(jnp.float32)[:, None, :]).astype(jnp.bfloat16).reshape(TOKENS * TOP, D)
    repeated = jnp.repeat(tokens, TOP, axis=0)
    total_slots = EXPERTS * sources * CAP
    slot_x = jnp.zeros((total_slots, D), jnp.bfloat16).at[slot_index].set(repeated).reshape(EXPERTS, sources * CAP, D)
    slot_c = jnp.zeros((total_slots, D), jnp.bfloat16).at[slot_index].set(scaled).reshape(EXPERTS, sources * CAP, D)

    def expert_pass(operands):
        token_rows, cot_rows = operands[0], operands[1]
        weights = operands[2:]
        hidden, part_gate, part_up, part_down = block_terms(weights, token_rows, cot_rows)
        expert_out = jnp.dot(hidden, weights[2], preferred_element_type=jnp.float32).astype(jnp.bfloat16)
        return expert_out, part_gate, part_up, part_down

    expert_out, hvp_gate, hvp_up, hvp_down = lax.map(expert_pass, (slot_x, slot_c, gate_weight, up_weight, down_weight, dir_gate, dir_up, dir_down))
    picked = expert_out.reshape(total_slots, D)[slot_index].astype(jnp.float32).reshape(TOKENS, TOP, D)
    mixed = jnp.sum(gate_prob[:, :, None] * picked, axis=1).astype(jnp.bfloat16)
    return (mixed, hvp_gate, hvp_up, hvp_down)
```

```python
import functools

import jax
import jax.numpy as jnp
from jax import lax
from jax.experimental import pallas as pl
from jax.experimental.pallas import tpu as pltpu
from jax.sharding import PartitionSpec as P

CHUNKS = 4
MESH = pl.DeviceIdType.MESH
VMEM = pl.BlockSpec(memory_space=pltpu.VMEM)


def meet(peers):
    barrier = pltpu.get_barrier_semaphore()
    for peer in peers:
        pl.semaphore_signal(barrier, inc=1, device_id=peer, device_id_type=MESH)
    pl.semaphore_wait(barrier, len(peers))


def send(src, dst, sems, slot, peer):
    send_sems, recv_sems = sems
    return pltpu.make_async_remote_copy(
        src_ref=src,
        dst_ref=dst,
        send_sem=send_sems.at[slot],
        recv_sem=recv_sems.at[slot],
        device_id=peer,
        device_id_type=MESH,
    )


def gather_kernel(
    chips, tok_ref, cot_ref, gate_ref, all_tok, all_cot, all_gate, *sems
):
    row, col = lax.axis_index("dp"), lax.axis_index("expert")
    chip, core = col // 2, col % 2
    side = row % 2
    other_row = row + 1 - 2 * side
    partner_col = col + 1 - 2 * core
    partner, beside = (row, partner_col), (other_row, col)
    experts = 2 * chips
    others = [(row, lax.rem(col + step, experts)) for step in range(1, experts)]
    meet(others + [beside])
    own, meta, far, near, relay = (sems[2 * i : 2 * i + 2] for i in range(5))
    half = tok_ref.shape[0] // 2
    part = half // CHUNKS
    pairs = ((tok_ref, all_tok), (cot_ref, all_cot))
    started = []
    arrivals = []

    for chunk in range(CHUNKS):
        for step in range(1, chips):
            peer = (row, lax.rem(chip + step, chips) * 2 + core)
            for which, (src, dst) in enumerate(pairs):
                rows = pl.ds(pl.multiple_of(side * half + chunk * part, part), part)
                slot = ((step - 1) * CHUNKS + chunk) * 2 + which
                copy = send(src.at[rows], dst.at[col, rows], far, slot, peer)
                copy.start()
                started.append(copy)
    for step, peer in enumerate(others):
        copy = send(gate_ref, all_gate.at[col], meta, step, peer)
        copy.start()
        started.append(copy)
        arrivals.append(copy)
    for which, (src, dst) in enumerate(pairs):
        copy = send(src, dst.at[col], own, which, partner)
        copy.start()
        started.append(copy)
        arrivals.append(copy)
    all_tok[pl.ds(col, 1)] = tok_ref[...][None]
    all_cot[pl.ds(col, 1)] = cot_ref[...][None]
    all_gate[pl.ds(col, 1)] = gate_ref[...][None]

    def pass_on(dst, block, rows, slot, source, both):
        send(dst.at[block, rows], dst.at[block, rows], source, slot, partner).wait_recv()
        index = slot * 2 + (0 if both else 1)
        onward = send(dst.at[block, rows], dst.at[block, rows], relay, index, partner)
        if both:
            across = send(dst.at[block, rows], dst.at[block, rows], near, slot, beside)
            across.start()
            started.append(across)
        onward.start()
        started.append(onward)
        arrivals.append(onward)

    for source, both, lag in ((far, True, 0), (near, False, 0)):
        for chunk in range(CHUNKS):
            for step in range(1, chips):
                block = lax.rem(chip + chips - step, chips) * 2 + core
                from_side = side if both else 1 - side
                rows = pl.ds(pl.multiple_of(from_side * half + chunk * part, part), part)
                for which, (_, dst) in enumerate(pairs):
                    slot = ((step - 1) * CHUNKS + chunk) * 2 + which
                    pass_on(dst, block, rows, slot, source, both)
    for copy in arrivals:
        copy.wait_recv()
    for copy in started:
        copy.wait_send()


def gather_blocks(tokens, cotangent, gates, chips):
    slots = max(1, (chips - 1) * CHUNKS * 2)
    experts = 2 * chips
    dma = pltpu.SemaphoreType.DMA
    counts = (2, experts - 1, slots, slots, 2 * slots)
    blocks = (experts,) + tokens.shape
    return pl.pallas_call(
        functools.partial(gather_kernel, chips),
        out_shape=(
            jax.ShapeDtypeStruct(blocks, tokens.dtype),
            jax.ShapeDtypeStruct(blocks, cotangent.dtype),
            jax.ShapeDtypeStruct((experts,) + gates.shape, gates.dtype),
        ),
        in_specs=[VMEM] * 3,
        out_specs=(VMEM,) * 3,
        scratch_shapes=[dma((count,)) for count in counts for _ in range(2)],
        compiler_params=pltpu.CompilerParams(
            collective_id=0, has_side_effects=True, vmem_limit_bytes=60 * 2**20
        ),
        name="gather_blocks",
    )(tokens, cotangent, gates)


def across(left, right):
    return lax.dot_general(left, right, (((1,), (1,)), ((), ())), preferred_element_type=jnp.float32)


def block_kernel(
    tok_ref, cot_ref, gate_ref, g_ref, u_ref, w_ref, vg_ref, vu_ref, vw_ref,
    hvp_g, hvp_u, hvp_w, out_ref, scaled, total,
):
    step = pl.program_id(0)

    @pl.when(step == 0)
    def _():
        scaled[...] = (gate_ref[...] * cot_ref[...].astype(jnp.float32)).astype(jnp.bfloat16)
        total[...] = jnp.zeros_like(total)

    tok, cot = tok_ref[...], scaled[...]
    a, b = across(g_ref[...], tok), across(u_ref[...], tok)
    ta, tb = across(vg_ref[...], tok), across(vu_ref[...], tok)
    q, tq = across(w_ref[...], cot), across(vw_ref[...], cot)
    s = jax.nn.sigmoid(a)
    g = a * s
    g1 = s * (1.0 + a * (1.0 - s))
    g2 = s * (1.0 - s) * (2.0 + a * (1.0 - 2.0 * s))
    tg = g1 * ta
    hidden = (g * b).astype(jnp.bfloat16)
    hidden_tang = (tg * b + g * tb).astype(jnp.bfloat16)
    resid_gate = ((tq * b + q * tb) * g1 + q * b * g2 * ta).astype(jnp.bfloat16)
    resid_up = (tq * g + q * tg).astype(jnp.bfloat16)
    total[...] += lax.dot_general(
        hidden, w_ref[...], (((0,), (0,)), ((), ())), preferred_element_type=jnp.float32
    )
    hvp_g[...] = jnp.dot(resid_gate, tok, preferred_element_type=jnp.float32)
    hvp_u[...] = jnp.dot(resid_up, tok, preferred_element_type=jnp.float32)
    hvp_w[...] = jnp.dot(hidden_tang, cot, preferred_element_type=jnp.float32)

    @pl.when(step == pl.num_programs(0) - 1)
    def _():
        out_ref[...] = (gate_ref[...] * total[...]).astype(jnp.bfloat16)


def block_terms(tokens, cotangent, gate, weights):
    rows, width = tokens.shape
    units = weights[0].shape[0]
    tile = max(n for n in range(16, units + 1, 16) if units % n == 0 and n * rows <= 224 * 512)
    whole = lambda shape: pl.BlockSpec(shape, lambda i: (0, 0))
    piece = pl.BlockSpec((tile, width), lambda i: (i, 0))
    out = jax.ShapeDtypeStruct((units, width), jnp.float32)
    return pl.pallas_call(
        block_kernel,
        grid=(units // tile,),
        out_shape=(out, out, out, jax.ShapeDtypeStruct((rows, width), jnp.bfloat16)),
        in_specs=[whole((rows, width)), whole((rows, width)), whole((rows, 1))] + [piece] * 6,
        out_specs=(piece, piece, piece, whole((rows, width))),
        scratch_shapes=[
            pltpu.VMEM((rows, width), jnp.bfloat16),
            pltpu.VMEM((rows, width), jnp.float32),
        ],
        compiler_params=pltpu.CompilerParams(
            dimension_semantics=("arbitrary",), vmem_limit_bytes=63 * 2**20
        ),
        name="block_terms",
    )(tokens, cotangent, gate, *weights)


def combine_kernel(
    chips, layers, part_ref, out_ref,
    from_core, core_sum, y_first, a_sum, x_last, x_first, b_sum, y_last, plane, from_z, share,
    gathered, from_partner, *sems,
):
    row, col = lax.axis_index("dp"), lax.axis_index("expert")
    chip, core = col // 2, col % 2
    layer, side = row // 2, row % 2
    partner = (row, col + 1 - 2 * core)
    beside = (row + 1 - 2 * side, col)
    chip_peers = [(row, lax.rem(chip + n, chips) * 2 + core) for n in range(1, chips)]
    layer_peers = [(lax.rem(layer + n, layers) * 2 + side, col) for n in range(1, layers)]
    meet([partner, beside] + chip_peers + layer_peers)
    core_s, ya_s, xa_s, xb_s, yb_s, z_s, gz_s, gx_s, back_s = (sems[2 * i : 2 * i + 2] for i in range(9))
    width = part_ref.shape[1]
    feats = width // 2
    wide, slim = feats // 2, feats // 4
    chip_rows = part_ref.shape[0] // chips
    rows_z = chip_rows // layers
    tok_dev = chip_rows // 2
    f32, bf16 = jnp.float32, jnp.bfloat16
    sent = []

    def go(src, dst, sems, slot, peer):
        copy = send(src, dst, sems, slot, peer)
        copy.start()
        sent.append(copy)
        return copy

    def cols(start, size):
        return pl.ds(pl.multiple_of(start, size), size)

    mine, theirs = cols(core * feats, feats), cols((1 - core) * feats, feats)
    my_slim, their_slim = cols(side * slim, slim), cols((1 - side) * slim, slim)
    my_rows = cols(chip * chip_rows, chip_rows)

    go(part_ref.at[:, theirs], from_core, core_s, 0, partner).wait_recv()
    core_sum[...] = (part_ref[:, mine].astype(f32) + from_core[...].astype(f32)).astype(bf16)

    late = wide + (1 - side) * slim
    x_copy = go(core_sum.at[:, cols(late, slim)], x_first, xb_s, 0, beside)
    y_copies = []
    for n, peer in enumerate(chip_peers):
        target = lax.rem(chip + n + 1, chips)
        source = core_sum.at[cols(target * chip_rows, chip_rows), pl.ds(0, wide)]
        y_copies.append(go(source, y_first.at[n], ya_s, n, peer))
    value = core_sum[my_rows, :wide].astype(f32)
    for n, copy in enumerate(y_copies):
        copy.wait_recv()
        value = value + y_first[n].astype(f32)
    a_sum[...] = value.astype(bf16)
    x_last_copy = go(a_sum.at[:, their_slim], x_last, xa_s, 0, beside)
    x_copy.wait_recv()
    b_sum[...] = (
        core_sum[:, cols(wide + side * slim, slim)].astype(f32) + x_first[...].astype(f32)
    ).astype(bf16)
    y_copies = []
    for n, peer in enumerate(chip_peers):
        target = lax.rem(chip + n + 1, chips)
        source = b_sum.at[cols(target * chip_rows, chip_rows)]
        y_copies.append(go(source, y_last.at[n], yb_s, n, peer))
    x_last_copy.wait_recv()
    plane[:, :slim] = (a_sum[:, my_slim].astype(f32) + x_last[...].astype(f32)).astype(bf16)
    value = b_sum[my_rows].astype(f32)
    for n, copy in enumerate(y_copies):
        copy.wait_recv()
        value = value + y_last[n].astype(f32)
    plane[:, slim:] = value.astype(bf16)

    z_copies = []
    for n, peer in enumerate(layer_peers):
        target = lax.rem(layer + n + 1, layers)
        z_copies.append(go(plane.at[cols(target * rows_z, rows_z)], from_z.at[n], z_s, n, peer))
    my_z = cols(layer * rows_z, rows_z)
    value = plane[my_z].astype(f32)
    for n, copy in enumerate(z_copies):
        copy.wait_recv()
        value = value + from_z[n].astype(f32)
    share[...] = value.astype(bf16)

    x_back = [go(share, gathered.at[side, my_z], gx_s, 0, beside)]
    z_back = []
    for n, peer in enumerate(layer_peers):
        z_back.append(go(share, gathered.at[side, my_z], gz_s, n, peer))
    gathered[pl.ds(side, 1), my_z] = share[...][None]
    for n, copy in enumerate(z_back):
        copy.wait_recv()
        origin = lax.rem(layer + layers - n - 1, layers)
        place = gathered.at[side, cols(origin * rows_z, rows_z)]
        x_back.append(go(place, place, gx_s, n + 1, beside))
    own_block, partner_block = cols(core * tok_dev, tok_dev), cols((1 - core) * tok_dev, tok_dev)
    back = [go(gathered.at[side, partner_block], from_partner.at[side], back_s, 0, partner)]
    for copy in x_back:
        copy.wait_recv()
    back.append(go(gathered.at[1 - side, partner_block], from_partner.at[1 - side], back_s, 1, partner))
    for group in range(2):
        for half in range(2):
            at = cols(core * feats + group * wide + half * slim, slim)
            out_ref[:, at] = gathered[half, own_block, group * slim : (group + 1) * slim]
    for copy in back:
        copy.wait_recv()
    for group in range(2):
        for half in range(2):
            at = cols((1 - core) * feats + group * wide + half * slim, slim)
            out_ref[:, at] = from_partner[half, :, group * slim : (group + 1) * slim]
    for copy in sent:
        copy.wait_send()


def combine(part, chips, layers):
    rows, width = part.shape
    feats = width // 2
    wide, slim = feats // 2, feats // 4
    chip_rows = rows // chips
    rows_z = chip_rows // layers
    tok_dev = chip_rows // 2
    dma = pltpu.SemaphoreType.DMA
    far, deep = max(1, chips - 1), max(1, layers - 1)
    counts = (1, far, 1, 1, far, deep, deep, layers, 2)
    held = lambda *shape: pltpu.VMEM(shape, jnp.bfloat16)
    return pl.pallas_call(
        functools.partial(combine_kernel, chips, layers),
        out_shape=jax.ShapeDtypeStruct((tok_dev, width), jnp.bfloat16),
        in_specs=[VMEM],
        out_specs=VMEM,
        scratch_shapes=[
            held(rows, feats),
            held(rows, feats),
            held(far, chip_rows, wide),
            held(chip_rows, wide),
            held(chip_rows, slim),
            held(rows, slim),
            held(rows, slim),
            held(far, chip_rows, slim),
            held(chip_rows, wide),
            held(deep, rows_z, wide),
            held(rows_z, wide),
            held(2, chip_rows, wide),
            held(2, tok_dev, wide),
        ]
        + [dma((count,)) for count in counts for _ in range(2)],
        compiler_params=pltpu.CompilerParams(
            collective_id=1, has_side_effects=True, vmem_limit_bytes=60 * 2**20
        ),
        name="combine",
    )(part)


def shards(tokens, cotangent, router_logits, routes, *weights):
    experts = lax.axis_size("expert")
    chips, layers = experts // 2, lax.axis_size("dp") // 2
    tok_dev, width = tokens.shape
    lines = -(-experts // 8) * 8
    logits, named = router_logits.T, routes.T
    first = jax.nn.sigmoid(logits[0] - logits[1])[None]
    number = jnp.arange(lines, dtype=jnp.int32)[:, None]
    gates = jnp.where(named[0][None] == number, first, 0.0) + jnp.where(
        named[1][None] == number, 1.0 - first, 0.0
    )
    all_tok, all_cot, all_gate = gather_blocks(tokens, cotangent, gates, chips)
    rows = experts * tok_dev
    own = lax.dynamic_index_in_dim(all_gate, lax.axis_index("expert"), 1, keepdims=False)
    hvp_gate, hvp_up, hvp_down, part = block_terms(
        all_tok.reshape(rows, width),
        all_cot.reshape(rows, width),
        own.reshape(rows, 1),
        [weight[0] for weight in weights],
    )
    mixed = combine(part, chips, layers)
    return (mixed, hvp_gate[None], hvp_up[None], hvp_down[None])


def solution(mesh):
    rows, units = P("expert", None), P("expert", "dp", None)
    return jax.shard_map(
        shards,
        mesh=mesh,
        in_specs=(rows,) * 4 + (units,) * 6,
        out_specs=(rows, units, units, units),
        check_vma=False,
    )
```

```python
import functools

import jax
import jax.numpy as jnp
from jax import lax
from jax.experimental import pallas as pl
from jax.experimental.pallas import tpu as pltpu
from jax.sharding import PartitionSpec as P

CHUNKS = 4
MESH = pl.DeviceIdType.MESH
VMEM = pl.BlockSpec(memory_space=pltpu.VMEM)


def meet(peers):
    barrier = pltpu.get_barrier_semaphore()
    for peer in peers:
        pl.semaphore_signal(barrier, inc=1, device_id=peer, device_id_type=MESH)
    pl.semaphore_wait(barrier, len(peers))


def send(src, dst, sems, slot, peer):
    send_sems, recv_sems = sems
    return pltpu.make_async_remote_copy(
        src_ref=src,
        dst_ref=dst,
        send_sem=send_sems.at[slot],
        recv_sem=recv_sems.at[slot],
        device_id=peer,
        device_id_type=MESH,
    )


def gather_kernel(
    chips, tok_ref, cot_ref, gate_ref, all_tok, all_cot, all_gate, *sems
):
    row, col = lax.axis_index("dp"), lax.axis_index("expert")
    chip, core = col // 2, col % 2
    side = row % 2
    other_row = row + 1 - 2 * side
    partner_col = col + 1 - 2 * core
    partner, beside = (row, partner_col), (other_row, col)
    experts = 2 * chips
    others = [(row, lax.rem(col + step, experts)) for step in range(1, experts)]
    meet(others + [beside])
    own, meta, far, near, relay = (sems[2 * i : 2 * i + 2] for i in range(5))
    half = tok_ref.shape[0] // 2
    part = half // CHUNKS
    pairs = ((tok_ref, all_tok), (cot_ref, all_cot))
    started = []
    arrivals = []

    for chunk in range(CHUNKS):
        for step in range(1, chips):
            peer = (row, lax.rem(chip + step, chips) * 2 + core)
            for which, (src, dst) in enumerate(pairs):
                rows = pl.ds(pl.multiple_of(side * half + chunk * part, part), part)
                slot = ((step - 1) * CHUNKS + chunk) * 2 + which
                copy = send(src.at[rows], dst.at[col, rows], far, slot, peer)
                copy.start()
                started.append(copy)
    for step, peer in enumerate(others):
        copy = send(gate_ref, all_gate.at[col], meta, step, peer)
        copy.start()
        started.append(copy)
        arrivals.append(copy)
    for which, (src, dst) in enumerate(pairs):
        copy = send(src, dst.at[col], own, which, partner)
        copy.start()
        started.append(copy)
        arrivals.append(copy)
    all_tok[pl.ds(col, 1)] = tok_ref[...][None]
    all_cot[pl.ds(col, 1)] = cot_ref[...][None]
    all_gate[pl.ds(col, 1)] = gate_ref[...][None]

    def pass_on(dst, block, rows, slot, source, both):
        send(dst.at[block, rows], dst.at[block, rows], source, slot, partner).wait_recv()
        index = slot * 2 + (0 if both else 1)
        onward = send(dst.at[block, rows], dst.at[block, rows], relay, index, partner)
        if both:
            across = send(dst.at[block, rows], dst.at[block, rows], near, slot, beside)
            across.start()
            started.append(across)
        onward.start()
        started.append(onward)
        arrivals.append(onward)

    for source, both, lag in ((far, True, 0), (near, False, 0)):
        for chunk in range(CHUNKS):
            for step in range(1, chips):
                block = lax.rem(chip + chips - step, chips) * 2 + core
                from_side = side if both else 1 - side
                rows = pl.ds(pl.multiple_of(from_side * half + chunk * part, part), part)
                for which, (_, dst) in enumerate(pairs):
                    slot = ((step - 1) * CHUNKS + chunk) * 2 + which
                    pass_on(dst, block, rows, slot, source, both)
    for copy in arrivals:
        copy.wait_recv()
    for copy in started:
        copy.wait_send()


def gather_blocks(tokens, cotangent, gates, chips):
    slots = max(1, (chips - 1) * CHUNKS * 2)
    experts = 2 * chips
    dma = pltpu.SemaphoreType.DMA
    counts = (2, experts - 1, slots, slots, 2 * slots)
    blocks = (experts,) + tokens.shape
    return pl.pallas_call(
        functools.partial(gather_kernel, chips),
        out_shape=(
            jax.ShapeDtypeStruct(blocks, tokens.dtype),
            jax.ShapeDtypeStruct(blocks, cotangent.dtype),
            jax.ShapeDtypeStruct((experts,) + gates.shape, gates.dtype),
        ),
        in_specs=[VMEM] * 3,
        out_specs=(VMEM,) * 3,
        scratch_shapes=[dma((count,)) for count in counts for _ in range(2)],
        compiler_params=pltpu.CompilerParams(
            collective_id=0, has_side_effects=True, vmem_limit_bytes=60 * 2**20
        ),
        name="gather_blocks",
    )(tokens, cotangent, gates)


def across(left, right):
    return lax.dot_general(left, right, (((1,), (1,)), ((), ())), preferred_element_type=jnp.float32)


def block_kernel(
    tok_ref, cot_ref, gate_ref, g_ref, u_ref, w_ref, vg_ref, vu_ref, vw_ref,
    hvp_g, hvp_u, hvp_w, out_ref, scaled, total,
):
    step = pl.program_id(0)

    @pl.when(step == 0)
    def _():
        scaled[...] = (gate_ref[...] * cot_ref[...].astype(jnp.float32)).astype(jnp.bfloat16)
        total[...] = jnp.zeros_like(total)

    tok, cot = tok_ref[...], scaled[...]
    stacked = jnp.concatenate([g_ref[...], u_ref[...], vg_ref[...], vu_ref[...]], axis=0)
    a, b, ta, tb = jnp.split(across(stacked, tok), 4, axis=0)
    q, tq = jnp.split(across(jnp.concatenate([w_ref[...], vw_ref[...]], axis=0), cot), 2, axis=0)
    s = jax.nn.sigmoid(a)
    g = a * s
    g1 = s * (1.0 + a * (1.0 - s))
    g2 = s * (1.0 - s) * (2.0 + a * (1.0 - 2.0 * s))
    tg = g1 * ta
    hidden = (g * b).astype(jnp.bfloat16)
    hidden_tang = (tg * b + g * tb).astype(jnp.bfloat16)
    resid_gate = ((tq * b + q * tb) * g1 + q * b * g2 * ta).astype(jnp.bfloat16)
    resid_up = (tq * g + q * tg).astype(jnp.bfloat16)
    total[...] += lax.dot_general(
        hidden, w_ref[...], (((0,), (0,)), ((), ())), preferred_element_type=jnp.float32
    )
    hvp_g[...] = jnp.dot(resid_gate, tok, preferred_element_type=jnp.float32)
    hvp_u[...] = jnp.dot(resid_up, tok, preferred_element_type=jnp.float32)
    hvp_w[...] = jnp.dot(hidden_tang, cot, preferred_element_type=jnp.float32)

    @pl.when(step == pl.num_programs(0) - 1)
    def _():
        out_ref[...] = (gate_ref[...] * total[...]).astype(jnp.bfloat16)


def block_terms(tokens, cotangent, gate, weights):
    rows, width = tokens.shape
    units = weights[0].shape[0]
    tile = max(n for n in range(16, units + 1, 16) if units % n == 0 and n * rows <= 224 * 512)
    whole = lambda shape: pl.BlockSpec(shape, lambda i: (0, 0))
    piece = pl.BlockSpec((tile, width), lambda i: (i, 0))
    out = jax.ShapeDtypeStruct((units, width), jnp.float32)
    return pl.pallas_call(
        block_kernel,
        grid=(units // tile,),
        out_shape=(out, out, out, jax.ShapeDtypeStruct((rows, width), jnp.bfloat16)),
        in_specs=[whole((rows, width)), whole((rows, width)), whole((rows, 1))] + [piece] * 6,
        out_specs=(piece, piece, piece, whole((rows, width))),
        scratch_shapes=[
            pltpu.VMEM((rows, width), jnp.bfloat16),
            pltpu.VMEM((rows, width), jnp.float32),
        ],
        compiler_params=pltpu.CompilerParams(
            dimension_semantics=("arbitrary",), vmem_limit_bytes=63 * 2**20
        ),
        name="block_terms",
    )(tokens, cotangent, gate, *weights)


def combine_kernel(
    chips, layers, part_ref, out_ref,
    from_core, core_sum, y_first, a_sum, x_last, x_first, b_sum, y_last, plane, from_z, share,
    gathered, from_partner, *sems,
):
    row, col = lax.axis_index("dp"), lax.axis_index("expert")
    chip, core = col // 2, col % 2
    layer, side = row // 2, row % 2
    partner = (row, col + 1 - 2 * core)
    beside = (row + 1 - 2 * side, col)
    chip_peers = [(row, lax.rem(chip + n, chips) * 2 + core) for n in range(1, chips)]
    layer_peers = [(lax.rem(layer + n, layers) * 2 + side, col) for n in range(1, layers)]
    meet([partner, beside] + chip_peers + layer_peers)
    core_s, ya_s, xa_s, xb_s, yb_s, z_s, gz_s, gx_s, back_s = (sems[2 * i : 2 * i + 2] for i in range(9))
    width = part_ref.shape[1]
    feats = width // 2
    wide, slim = feats // 2, feats // 4
    chip_rows = part_ref.shape[0] // chips
    rows_z = chip_rows // layers
    tok_dev = chip_rows // 2
    f32, bf16 = jnp.float32, jnp.bfloat16
    sent = []

    def go(src, dst, sems, slot, peer):
        copy = send(src, dst, sems, slot, peer)
        copy.start()
        sent.append(copy)
        return copy

    def cols(start, size):
        return pl.ds(pl.multiple_of(start, size), size)

    mine, theirs = cols(core * feats, feats), cols((1 - core) * feats, feats)
    my_slim, their_slim = cols(side * slim, slim), cols((1 - side) * slim, slim)
    my_rows = cols(chip * chip_rows, chip_rows)

    go(part_ref.at[:, theirs], from_core, core_s, 0, partner).wait_recv()
    core_sum[...] = (part_ref[:, mine].astype(f32) + from_core[...].astype(f32)).astype(bf16)

    late = wide + (1 - side) * slim
    x_copy = go(core_sum.at[:, cols(late, slim)], x_first, xb_s, 0, beside)
    y_copies = []
    for n, peer in enumerate(chip_peers):
        target = lax.rem(chip + n + 1, chips)
        source = core_sum.at[cols(target * chip_rows, chip_rows), pl.ds(0, wide)]
        y_copies.append(go(source, y_first.at[n], ya_s, n, peer))
    value = core_sum[my_rows, :wide].astype(f32)
    for n, copy in enumerate(y_copies):
        copy.wait_recv()
        value = value + y_first[n].astype(f32)
    a_sum[...] = value.astype(bf16)
    x_last_copy = go(a_sum.at[:, their_slim], x_last, xa_s, 0, beside)
    x_copy.wait_recv()
    b_sum[...] = (
        core_sum[:, cols(wide + side * slim, slim)].astype(f32) + x_first[...].astype(f32)
    ).astype(bf16)
    y_copies = []
    for n, peer in enumerate(chip_peers):
        target = lax.rem(chip + n + 1, chips)
        source = b_sum.at[cols(target * chip_rows, chip_rows)]
        y_copies.append(go(source, y_last.at[n], yb_s, n, peer))
    x_last_copy.wait_recv()
    plane[:, :slim] = (a_sum[:, my_slim].astype(f32) + x_last[...].astype(f32)).astype(bf16)
    value = b_sum[my_rows].astype(f32)
    for n, copy in enumerate(y_copies):
        copy.wait_recv()
        value = value + y_last[n].astype(f32)
    plane[:, slim:] = value.astype(bf16)

    z_copies = []
    for n, peer in enumerate(layer_peers):
        target = lax.rem(layer + n + 1, layers)
        z_copies.append(go(plane.at[cols(target * rows_z, rows_z)], from_z.at[n], z_s, n, peer))
    my_z = cols(layer * rows_z, rows_z)
    value = plane[my_z].astype(f32)
    for n, copy in enumerate(z_copies):
        copy.wait_recv()
        value = value + from_z[n].astype(f32)
    share[...] = value.astype(bf16)

    x_back = [go(share, gathered.at[side, my_z], gx_s, 0, beside)]
    z_back = []
    for n, peer in enumerate(layer_peers):
        z_back.append(go(share, gathered.at[side, my_z], gz_s, n, peer))
    gathered[pl.ds(side, 1), my_z] = share[...][None]
    for n, copy in enumerate(z_back):
        copy.wait_recv()
        origin = lax.rem(layer + layers - n - 1, layers)
        place = gathered.at[side, cols(origin * rows_z, rows_z)]
        x_back.append(go(place, place, gx_s, n + 1, beside))
    own_block, partner_block = cols(core * tok_dev, tok_dev), cols((1 - core) * tok_dev, tok_dev)
    back = [go(gathered.at[side, partner_block], from_partner.at[side], back_s, 0, partner)]
    for copy in x_back:
        copy.wait_recv()
    back.append(go(gathered.at[1 - side, partner_block], from_partner.at[1 - side], back_s, 1, partner))
    for group in range(2):
        for half in range(2):
            at = cols(core * feats + group * wide + half * slim, slim)
            out_ref[:, at] = gathered[half, own_block, group * slim : (group + 1) * slim]
    for copy in back:
        copy.wait_recv()
    for group in range(2):
        for half in range(2):
            at = cols((1 - core) * feats + group * wide + half * slim, slim)
            out_ref[:, at] = from_partner[half, :, group * slim : (group + 1) * slim]
    for copy in sent:
        copy.wait_send()


def combine(part, chips, layers):
    rows, width = part.shape
    feats = width // 2
    wide, slim = feats // 2, feats // 4
    chip_rows = rows // chips
    rows_z = chip_rows // layers
    tok_dev = chip_rows // 2
    dma = pltpu.SemaphoreType.DMA
    far, deep = max(1, chips - 1), max(1, layers - 1)
    counts = (1, far, 1, 1, far, deep, deep, layers, 2)
    held = lambda *shape: pltpu.VMEM(shape, jnp.bfloat16)
    return pl.pallas_call(
        functools.partial(combine_kernel, chips, layers),
        out_shape=jax.ShapeDtypeStruct((tok_dev, width), jnp.bfloat16),
        in_specs=[VMEM],
        out_specs=VMEM,
        scratch_shapes=[
            held(rows, feats),
            held(rows, feats),
            held(far, chip_rows, wide),
            held(chip_rows, wide),
            held(chip_rows, slim),
            held(rows, slim),
            held(rows, slim),
            held(far, chip_rows, slim),
            held(chip_rows, wide),
            held(deep, rows_z, wide),
            held(rows_z, wide),
            held(2, chip_rows, wide),
            held(2, tok_dev, wide),
        ]
        + [dma((count,)) for count in counts for _ in range(2)],
        compiler_params=pltpu.CompilerParams(
            collective_id=1, has_side_effects=True, vmem_limit_bytes=60 * 2**20
        ),
        name="combine",
    )(part)


def shards(tokens, cotangent, router_logits, routes, *weights):
    experts = lax.axis_size("expert")
    chips, layers = experts // 2, lax.axis_size("dp") // 2
    tok_dev, width = tokens.shape
    lines = -(-experts // 8) * 8
    logits, named = router_logits.T, routes.T
    first = jax.nn.sigmoid(logits[0] - logits[1])[None]
    number = jnp.arange(lines, dtype=jnp.int32)[:, None]
    gates = jnp.where(named[0][None] == number, first, 0.0) + jnp.where(
        named[1][None] == number, 1.0 - first, 0.0
    )
    all_tok, all_cot, all_gate = gather_blocks(tokens, cotangent, gates, chips)
    rows = experts * tok_dev
    own = lax.dynamic_index_in_dim(all_gate, lax.axis_index("expert"), 1, keepdims=False)
    hvp_gate, hvp_up, hvp_down, part = block_terms(
        all_tok.reshape(rows, width),
        all_cot.reshape(rows, width),
        own.reshape(rows, 1),
        [weight[0] for weight in weights],
    )
    mixed = combine(part, chips, layers)
    return (mixed, hvp_gate[None], hvp_up[None], hvp_down[None])


def solution(mesh):
    rows, units = P("expert", None), P("expert", "dp", None)
    return jax.shard_map(
        shards,
        mesh=mesh,
        in_specs=(rows,) * 4 + (units,) * 6,
        out_specs=(rows, units, units, units),
        check_vma=False,
    )
```
